32 devices in a mesh: seq: 8 (over z, y), head: 4 (over x, core).
Axes of the slice: x: 2, y: 2, z: 4, core: 2. Of those that a mesh axis runs over, the one named last changes fastest.
Arguments:
- patches: bfloat16 [2048, 1280], P('seq'), may hold values from -6 to 6
- norm_gain: float32 [1280], replicated, may hold values from 0.5 to 1.5
- w_qkv: bfloat16 [1280, 3, 1280], P('seq', None, 'head'), as said below
- w_out: bfloat16 [1280, 1280], P('head', 'seq'), may hold values from -0.15625 to 0.15625
- window_order: int32 [8, 64], P('seq'), may hold values from 0 to 63, each once within a row
- merge_gain: float32 [1280], replicated, may hold values from 0.5 to 1.5
- w_kv: bfloat16 [5120, 2, 1024], P('seq', None, 'head'), as said below
- queries: bfloat16 [16, 8192], P('seq', 'head'), may hold values from -6 to 6
- suffix_kv: bfloat16 [16, 64, 2, 1024], P('seq', None, None, 'head'), may hold values from -12 to 12
- question_lengths: int32 [16], P('seq'), may hold values from 1 to 64
- frame_range: int32 [16, 2], replicated, may hold values from 0 to 8, as said below
Outputs:
- answers: bfloat16 [16, 8192], P('seq', 'head')
The draws below stay inside these ranges and needn't reach their ends.
Inputs may be any that keep to these rules, and one draw needn't show every extreme that they name: `window_order`: each row is an ordering of a frame's units; positions w * 16 to (w + 1) * 16 - 1 form window w. `frame_range`: the first entry of a row is below the second. `w_qkv`: entries of order one over the square root of 1280. `w_kv`: entries of order one over the square root of 5120.
All inputs are finite; a program needn't handle non-finite values.
Results may differ from the reference program's by a relative error of at most 0.007.
Values may be sent and summed in bfloat16 or wider, within the bound.
A program may use at most 64 MiB of HBM per device.

```python
import math
import jax
import jax.numpy as jnp
from jax import lax

VD = 1280
VH = 16
QH = 64
KVH = 8
HD = 128
FPATCH = 256
WIN = 64
SUF = 64
FRAMES = 8
PATCHES = 2048
QUESTIONS = 16


def draw_frame_range(key, part):
    first_key, second_key = jax.random.split(jax.random.fold_in(key, 11))
    first_pick = jax.random.randint(first_key, (QUESTIONS,), 0, FRAMES)
    second_pick = jax.random.randint(second_key, (QUESTIONS,), 0, FRAMES)
    lower = jnp.minimum(first_pick, second_pick)
    upper = jnp.maximum(first_pick, second_pick) + 1
    return jnp.stack([lower, upper], axis=1).astype(jnp.int32)


def sign_vector(seed_key, count):
    return jnp.where(jax.random.bernoulli(seed_key, 0.5, (count,)), 1.0, -1.0).astype(jnp.float32)


def plant_plan(seed_key):
    subkeys = jax.random.split(jax.random.fold_in(seed_key, 29), 6)
    vision_levels = jnp.linspace(100.0, 400.0, VH)
    prefix_levels = jnp.linspace(100.0, 480.0, KVH)
    head_width = VD // VH
    vision_alpha = jnp.sqrt(jax.random.permutation(subkeys[0], vision_levels) / (VD * math.sqrt(head_width)))
    prefix_alpha = jax.random.permutation(subkeys[1], prefix_levels) / (6.0 * math.sqrt(4 * VD * HD))
    vision_sign = sign_vector(subkeys[2], VD)
    vision_dir = sign_vector(subkeys[3], VD)
    prefix_sign = sign_vector(subkeys[4], 4 * VD)
    prefix_dir = sign_vector(subkeys[5], KVH * HD)
    return (vision_alpha, vision_sign, vision_dir, prefix_alpha, prefix_sign, prefix_dir)


def draw_patches(key, part):
    vision_alpha, vision_sign, vision_dir, prefix_alpha, prefix_sign, prefix_dir = plant_plan(key)
    subkeys = jax.random.split(jax.random.fold_in(key, 37), 9)
    background = jnp.clip(jax.random.normal(subkeys[1], (PATCHES, VD), jnp.float32), -6.0, 6.0)
    unit_count = FPATCH // 4
    frame_keys = jax.random.split(subkeys[2], FRAMES)
    chosen = jax.vmap(lambda frame_key: jax.random.permutation(frame_key, unit_count)[:3])(frame_keys)
    vision_field = jax.random.uniform(subkeys[3], (FRAMES, 1, VD), jnp.float32)
    vision_noise = jnp.clip(jax.random.normal(subkeys[4], (FRAMES, 1, VD), jnp.float32), -6.0, 6.0)
    vision_base = jax.random.uniform(subkeys[5], (FRAMES, 1, 1), jnp.float32, 0.0, 0.2)
    thresholds = vision_base + 0.01 * jnp.arange(4, dtype=jnp.float32).reshape(1, 4, 1)
    vision_unit = jnp.where(vision_field < thresholds, vision_noise, 6.0 * vision_sign.reshape(1, 1, VD))
    prefix_field = jax.random.uniform(subkeys[6], (FRAMES, 4, VD), jnp.float32)
    prefix_noise = jnp.clip(jax.random.normal(subkeys[7], (FRAMES, 4, VD), jnp.float32), -6.0, 6.0)
    prefix_base = jax.random.uniform(subkeys[8], (FRAMES, 1, 1), jnp.float32, 0.0, 0.25)
    pattern = 6.0 * prefix_sign.reshape(1, 4, VD)
    first_unit = jnp.where(prefix_field < prefix_base, prefix_noise, pattern)
    second_unit = jnp.where(prefix_field < prefix_base + 0.01, prefix_noise, pattern)
    frame_ids = jnp.arange(FRAMES)
    layout = background.reshape(FRAMES, unit_count, 4, VD)
    layout = layout.at[frame_ids, chosen[:, 0]].set(vision_unit)
    layout = layout.at[frame_ids, chosen[:, 1]].set(first_unit)
    layout = layout.at[frame_ids, chosen[:, 2]].set(second_unit)
    return layout.reshape(PATCHES, VD).astype(jnp.bfloat16)


def draw_w_qkv(key, part):
    vision_alpha, vision_sign, vision_dir, prefix_alpha, prefix_sign, prefix_dir = plant_plan(key)
    weight_key = jax.random.fold_in(key, 41)
    random_part = jnp.clip(jax.random.normal(weight_key, (VD, 3, VD), jnp.float32), -4.0, 4.0) * VD ** (-0.5)
    column_alpha = jnp.repeat(vision_alpha, VD // VH)
    rank_one = vision_sign[:, None] * (column_alpha * vision_dir)[None, :] * VD ** (-0.5)
    planted = jnp.stack([rank_one, rank_one, jnp.zeros_like(rank_one)], axis=1)
    return (random_part + planted).astype(jnp.bfloat16)


def draw_w_kv(key, part):
    vision_alpha, vision_sign, vision_dir, prefix_alpha, prefix_sign, prefix_dir = plant_plan(key)
    weight_key = jax.random.fold_in(key, 43)
    random_part = jnp.clip(jax.random.normal(weight_key, (4 * VD, 2, KVH * HD), jnp.float32), -4.0, 4.0) * (4 * VD) ** (-0.5)
    column_alpha = jnp.repeat(prefix_alpha, HD)
    rank_one = prefix_sign[:, None] * (column_alpha * prefix_dir)[None, :] * (4 * VD) ** (-0.5)
    planted = jnp.stack([rank_one, jnp.zeros_like(rank_one)], axis=1)
    return (random_part + planted).astype(jnp.bfloat16)


def draw_queries(key, part):
    vision_alpha, vision_sign, vision_dir, prefix_alpha, prefix_sign, prefix_dir = plant_plan(key)
    subkeys = jax.random.split(jax.random.fold_in(key, 47), 3)
    background = jnp.clip(jax.random.normal(subkeys[0], (QUESTIONS, QH, HD), jnp.float32), -6.0, 6.0)
    chosen = jax.random.bernoulli(subkeys[1], 0.25, (QUESTIONS, QH))
    levels = jnp.array([1.5, 3.0, 6.0, 6.0], jnp.float32)
    strength = levels[jax.random.randint(subkeys[2], (QUESTIONS, QH), 0, 4)]
    direction = jnp.broadcast_to(prefix_dir.reshape(KVH, 1, HD), (KVH, QH // KVH, HD)).reshape(QH, HD)
    planted = strength[..., None] * direction[None]
    shaped = jnp.where(chosen[..., None], planted, background)
    return shaped.reshape(QUESTIONS, QH * HD).astype(jnp.bfloat16)


def touch_ends(entries, stream_key, low, largest):
    shape = entries.shape
    place = [jax.random.randint(jax.random.fold_in(stream_key, axis), (), 0, shape[axis]) for axis in range(len(shape))]
    entries = entries.at[tuple(place)].set(low)
    longest = shape.index(max(shape))
    place[longest] = (place[longest] + 1) % shape[longest]
    return entries.at[tuple(place)].set(largest)


def level_of(rng, shape, shards, least, largest):
    level = 1.0
    for axis_at, shards_of in shards:
        heights = jax.random.uniform(jax.random.fold_in(jax.random.fold_in(rng, 6), axis_at), (shards_of,), jnp.float32, least / len(shards), largest / len(shards))
        level = level * jnp.repeat(jnp.exp(heights), shape[axis_at] // shards_of).reshape((-1,) + (1,) * (len(shape) - 1 - axis_at))
    return level


def normal_values(key, dims, deviation, limit, pieces=(), held_as=jnp.bfloat16):
    entries = deviation * jax.random.normal(key, dims, jnp.float32)
    if pieces:
        entries = entries * level_of(key, dims, pieces, -0.22, 0.18)
    return jnp.clip(entries, -limit, limit).astype(held_as)


def setup_inputs(seed: int = 0) -> dict:
    key_list = jax.random.split(jax.random.key(seed), 12)
    patches = draw_patches(jax.random.fold_in(key_list[11], 71), 0)
    norm_gain = jnp.clip(1.0 + 0.1 * jax.random.normal(key_list[1], (VD,), jnp.float32), 0.5, 1.5)
    w_qkv = draw_w_qkv(jax.random.fold_in(key_list[11], 71), 0)
    w_out = normal_values(key_list[3], (VD, VD), VD ** -0.5, 0.15625, ((0, 4), (1, 8)))
    window_order = jax.vmap(lambda own: jax.random.permutation(own, FPATCH // 4))(jax.random.split(key_list[4], FRAMES)).reshape((FRAMES, FPATCH // 4)).astype(jnp.int32)
    merge_gain = jnp.clip(1.0 + 0.1 * jax.random.normal(key_list[5], (VD,), jnp.float32), 0.5, 1.5)
    w_kv = draw_w_kv(jax.random.fold_in(key_list[11], 71), 0)
    queries = draw_queries(jax.random.fold_in(key_list[11], 71), 0)
    suffix_kv = normal_values(key_list[8], (QUESTIONS, SUF, 2, KVH * HD), 2.0, 12.0, ((0, 8), (3, 4)))
    question_lengths = touch_ends(jax.random.randint(key_list[9], (QUESTIONS,), 1, SUF + 1), jax.random.fold_in(key_list[9], 1), 1, SUF).astype(jnp.int32)
    frame_range = draw_frame_range(jax.random.fold_in(key_list[11], 71), 0)
    return {"patches": patches, "norm_gain": norm_gain, "w_qkv": w_qkv, "w_out": w_out, "window_order": window_order, "merge_gain": merge_gain, "w_kv": w_kv, "queries": queries, "suffix_kv": suffix_kv, "question_lengths": question_lengths, "frame_range": frame_range}


def rms_scale(values, gain):
    return values * lax.rsqrt(lax.optimization_barrier(jnp.mean(values * values, axis=-1, keepdims=True)) + 1e-06) * gain

def reference(patches, norm_gain, w_qkv, w_out, window_order, merge_gain, w_kv, queries, suffix_kv, question_lengths, frame_range):
    head_size = VD // VH
    source = patches.astype(jnp.float32)
    normed = rms_scale(source, norm_gain).astype(jnp.bfloat16)
    projected = jnp.dot(normed, w_qkv.reshape(VD, 3 * VD), preferred_element_type=jnp.float32).astype(jnp.bfloat16)
    projected = projected.reshape(FRAMES, FPATCH // 4, 4, 3, VD)

    def frame_window(inputs):
        frame_rows, unit_order = inputs
        grouped = frame_rows[unit_order].reshape(-1, WIN, 3, VH, head_size).astype(jnp.float32)
        scores = jnp.einsum('wqhd,wkhd->whqk', grouped[:, :, 0], grouped[:, :, 1]) * head_size ** (-0.5)
        weights = jax.nn.softmax(scores, axis=-1).astype(jnp.bfloat16)
        weights = lax.optimization_barrier(weights).astype(jnp.float32)
        mixed = jnp.einsum('whqk,wkhd->wqhd', weights, grouped[:, :, 2]).astype(jnp.bfloat16)
        mixed = mixed.reshape(FPATCH // 4, 4, VD)
        return jnp.zeros_like(mixed).at[unit_order].set(mixed)
    attended = lax.map(frame_window, (projected, window_order)).reshape(PATCHES, VD)
    hidden = source + jnp.dot(attended, w_out, preferred_element_type=jnp.float32)
    merged = rms_scale(hidden, merge_gain).astype(jnp.bfloat16).reshape(PATCHES // 4, 4 * VD)
    visual = jnp.dot(merged, w_kv.reshape(4 * VD, 2 * KVH * HD), preferred_element_type=jnp.float32).astype(jnp.bfloat16)
    visual = visual.reshape(PATCHES // 4, 2, KVH, HD).astype(jnp.float32)
    prefix_keys = visual[:, 0]
    prefix_values = visual[:, 1]
    frame_index = jnp.arange(PATCHES // 4) // (FPATCH // 4)
    group = QH // KVH

    def answer(inputs):
        query_row, suffix_rows, length, bounds = inputs
        asking = query_row.reshape(KVH, group, HD).astype(jnp.float32)
        suffix_rows = suffix_rows.reshape(SUF, 2, KVH, HD).astype(jnp.float32)
        keys = jnp.concatenate([prefix_keys, suffix_rows[:, 0]], axis=0)
        values = jnp.concatenate([prefix_values, suffix_rows[:, 1]], axis=0)
        live = jnp.concatenate([(frame_index >= bounds[0]) & (frame_index < bounds[1]), jnp.arange(SUF) < length])
        scores = jnp.einsum('gjd,ngd->gjn', asking, keys) * HD ** (-0.5)
        scores = jnp.where(live[None, None, :], scores, -jnp.inf)
        weights = jnp.exp(scores - lax.optimization_barrier(jnp.max(scores, axis=-1, keepdims=True)))
        totals = lax.optimization_barrier(jnp.sum(weights, axis=-1))
        rounded = lax.optimization_barrier(weights.astype(jnp.bfloat16)).astype(jnp.float32)
        mixed = jnp.einsum('gjn,ngd->gjd', rounded, values) / totals[..., None]
        return mixed.reshape(QH * HD).astype(jnp.bfloat16)
    return lax.map(answer, (queries, suffix_kv, question_lengths, frame_range))
```

```python
import functools

import jax
import jax.numpy as jnp
from jax import lax
from jax.experimental import pallas as pl
from jax.experimental.pallas import tpu as pltpu
from jax.sharding import PartitionSpec as P

VD = 1280
VH = 16
HD = 128
FPATCH = 256
WIN = 64

MESH = pl.DeviceIdType.MESH
VMEM = pl.BlockSpec(memory_space=pltpu.VMEM)


def rms_scale(values, gain):
    return values * lax.rsqrt(jnp.mean(values * values, axis=-1, keepdims=True) + 1e-06) * gain


def exchange_kernel(axis, count, gather, x_ref, out_ref, send_sem, recv_sem, own_sem):
    me = lax.axis_index(axis)
    barrier = pltpu.get_barrier_semaphore()
    for step in range(1, count):
        pl.semaphore_signal(
            barrier, inc=1, device_id={axis: lax.rem(me + step, count)}, device_id_type=MESH
        )
    pl.semaphore_wait(barrier, count - 1)
    copies = []
    for step in range(1, count):
        peer = lax.rem(me + step, count)
        copy = pltpu.make_async_remote_copy(
            src_ref=x_ref if gather else x_ref.at[peer],
            dst_ref=out_ref.at[me],
            send_sem=send_sem.at[step],
            recv_sem=recv_sem.at[step],
            device_id={axis: peer},
            device_id_type=MESH,
        )
        copy.start()
        copies.append(copy)
    own = pltpu.make_async_copy(x_ref if gather else x_ref.at[me], out_ref.at[me], own_sem)
    own.start()
    own.wait()
    for copy in copies:
        copy.wait()


def exchange(x, axis, gather, collective_id):
    count = lax.axis_size(axis)
    shape = ((count,) + x.shape) if gather else x.shape
    return pl.pallas_call(
        functools.partial(exchange_kernel, axis, count, gather),
        out_shape=jax.ShapeDtypeStruct(shape, x.dtype),
        in_specs=[VMEM],
        out_specs=VMEM,
        scratch_shapes=[
            pltpu.SemaphoreType.DMA((count,)),
            pltpu.SemaphoreType.DMA((count,)),
            pltpu.SemaphoreType.DMA,
        ],
        compiler_params=pltpu.CompilerParams(collective_id=collective_id, has_side_effects=True),
        name=f"exchange_{collective_id}",
    )(x)


def ring_kernel(count, qkv_ref, wout_ref, qkv_out, wout_out, send_sem, recv_sem, own_sem):
    me = lax.axis_index("seq")
    odd = lax.rem(me, 2)
    place = (1 - odd) * (me // 2) + odd * (count - 1 - me // 2)

    def index_of(position):
        position = lax.rem(position + count, count)
        late = position // (count // 2)
        return (1 - late) * 2 * position + late * (2 * (count - 1 - position) + 1)

    neighbours = (index_of(place + 1), index_of(place - 1))
    barrier = pltpu.get_barrier_semaphore()
    for neighbour in neighbours:
        pl.semaphore_signal(barrier, inc=1, device_id={"seq": neighbour}, device_id_type=MESH)
    pl.semaphore_wait(barrier, 2)
    far, near = count // 2, count - 1 - count // 2
    pieces = 4

    def slot(piece, source):
        return qkv_out.at[piece, source] if piece < 3 else wout_out.at[source]

    def own(piece):
        return qkv_ref.at[piece] if piece < 3 else wout_ref

    copies = {}
    for step in range(far):
        for piece in range(pieces):
            for way in range(2):
                hops = far if (piece < 2) == (way == 0) else near
                if step >= hops:
                    continue
                source = index_of(place - step if way == 0 else place + step)
                if step > 0:
                    copies[step - 1, piece, way].wait_recv()
                copy = pltpu.make_async_remote_copy(
                    src_ref=own(piece) if step == 0 else slot(piece, source),
                    dst_ref=slot(piece, source),
                    send_sem=send_sem.at[step, piece, way],
                    recv_sem=recv_sem.at[step, piece, way],
                    device_id={"seq": neighbours[way]},
                    device_id_type=MESH,
                )
                copy.start()
                copies[step, piece, way] = copy
    kept = [pltpu.make_async_copy(own(p), slot(p, me), own_sem.at[p]) for p in range(pieces)]
    for copy in kept:
        copy.start()
    for copy in kept:
        copy.wait()
    for (step, piece, way), copy in copies.items():
        if (step + 1, piece, way) not in copies:
            copy.wait_recv()
    for copy in copies.values():
        copy.wait_send()


def ring_weights(w_qkv, w_out):
    count = lax.axis_size("seq")
    far = count // 2
    return pl.pallas_call(
        functools.partial(ring_kernel, count),
        out_shape=(
            jax.ShapeDtypeStruct((3, count) + w_qkv.shape[1:], w_qkv.dtype),
            jax.ShapeDtypeStruct((count,) + w_out.shape, w_out.dtype),
        ),
        in_specs=[VMEM, VMEM],
        out_specs=(VMEM, VMEM),
        scratch_shapes=[
            pltpu.SemaphoreType.DMA((far, 4, 2)),
            pltpu.SemaphoreType.DMA((far, 4, 2)),
            pltpu.SemaphoreType.DMA((4,)),
        ],
        compiler_params=pltpu.CompilerParams(collective_id=0, has_side_effects=True),
        name="ring_weights",
    )(w_qkv, w_out)


def frame_attention(query, key, value, unit_order, head_size):
    unit_count = unit_order.shape[0]
    patch_count = unit_count * 4
    ranks = jnp.sum(
        jnp.where(
            unit_order[None, :] == (jnp.arange(patch_count) // 4)[:, None],
            jnp.arange(unit_count)[None, :] // (WIN // 4),
            0,
        ),
        axis=1,
    )
    same = ranks[:, None] == ranks[None, :]
    scores = jnp.einsum(
        "qhd,khd->hqk", query, key, preferred_element_type=jnp.float32
    ) * head_size ** (-0.5)
    scores = jnp.where(same[None], scores, -jnp.inf)
    weights = jax.nn.softmax(scores, axis=-1).astype(jnp.bfloat16)
    return jnp.einsum(
        "hqk,khd->qhd", weights, value, preferred_element_type=jnp.float32
    ).astype(jnp.bfloat16)


def on_device(
    patches,
    norm_gain,
    w_qkv,
    w_out,
    window_order,
    merge_gain,
    w_kv,
    queries,
    suffix_kv,
    question_lengths,
    frame_range,
):
    head_count = lax.axis_size("head")
    seq_count = lax.axis_size("seq")
    row_count = patches.shape[0]
    frame_count = window_order.shape[0]
    columns = w_qkv.shape[2]
    head_size = VD // VH
    local_heads = columns // head_size
    source = patches.astype(jnp.float32)
    normed = rms_scale(source, norm_gain).astype(jnp.bfloat16)
    qkv_all, w_out_all = ring_weights(w_qkv.transpose(1, 0, 2), w_out)
    qkv_all = qkv_all.reshape(3, -1, columns)
    query, key, value = [
        jnp.dot(normed, qkv_all[part], preferred_element_type=jnp.float32)
        .astype(jnp.bfloat16)
        .reshape(frame_count, -1, local_heads, head_size)
        for part in range(3)
    ]
    attended = jax.vmap(
        lambda q, k, v, order: frame_attention(q, k, v, order, head_size)
    )(query, key, value, window_order).reshape(row_count, columns)
    w_full = w_out_all.transpose(1, 0, 2).reshape(columns, VD)
    share_rows = row_count // head_count
    partial = jnp.dot(attended, w_full, preferred_element_type=jnp.float32).astype(jnp.bfloat16)
    parts = exchange(partial.reshape(head_count, share_rows, VD), "head", False, 1)
    shared = jnp.sum(parts.astype(jnp.float32), axis=0)
    own_rows = lax.dynamic_slice_in_dim(source, lax.axis_index("head") * share_rows, share_rows, 0)
    merged = rms_scale(own_rows + shared, merge_gain).astype(jnp.bfloat16)
    share_tokens = share_rows // 4
    depth = w_kv.shape[0]
    merged = merged.reshape(share_tokens, seq_count, depth).transpose(1, 0, 2)
    merged = exchange(merged, "seq", False, 2)
    merged = exchange(merged, "head", True, 3)
    merged = merged.transpose(1, 0, 2, 3).reshape(-1, depth)
    kv_columns = w_kv.shape[2]
    partial = jnp.dot(
        merged, w_kv.reshape(depth, 2 * kv_columns), preferred_element_type=jnp.float32
    )
    parts = exchange(partial.reshape(seq_count, -1, 2 * kv_columns), "seq", False, 4)
    visual = jnp.sum(parts, axis=0).astype(jnp.bfloat16)
    visual = exchange(visual, "seq", True, 5).reshape(-1, 2 * kv_columns)

    token_count = visual.shape[0]
    quest_count = queries.shape[0]
    span = suffix_kv.shape[1]
    kv_local = kv_columns // HD
    asking = queries.reshape(quest_count, kv_local, -1, HD)
    frame_tokens = FPATCH // 4
    seq_index = lax.axis_index("seq")
    bounds = lax.dynamic_slice_in_dim(frame_range, seq_index * quest_count, quest_count, 0)
    frame_index = jnp.arange(token_count) // frame_tokens
    live = (frame_index[None, :] >= bounds[:, 0:1]) & (frame_index[None, :] < bounds[:, 1:2])
    suffix_live = jnp.arange(span)[None, :] < question_lengths[:, None]
    suffix = suffix_kv.reshape(quest_count, span, 2, kv_local, HD)
    answers = []
    for g in range(kv_local):
        ask = asking[:, g]
        keys = visual[:, g * HD : (g + 1) * HD]
        values = visual[:, kv_columns + g * HD : kv_columns + (g + 1) * HD]
        scores = jnp.einsum(
            "qjd,nd->qjn", ask, keys, preferred_element_type=jnp.float32
        ) * HD ** (-0.5)
        scores = jnp.where(live[:, None, :], scores, -jnp.inf)
        tail = jnp.einsum(
            "qjd,qsd->qjs", ask, suffix[:, :, 0, g], preferred_element_type=jnp.float32
        ) * HD ** (-0.5)
        tail = jnp.where(suffix_live[:, None, :], tail, -jnp.inf)
        highest = jnp.maximum(
            jnp.max(scores, axis=-1, keepdims=True), jnp.max(tail, axis=-1, keepdims=True)
        )
        weights = jnp.exp(scores - highest)
        tail_weights = jnp.exp(tail - highest)
        totals = jnp.sum(weights, axis=-1, keepdims=True) + jnp.sum(
            tail_weights, axis=-1, keepdims=True
        )
        mixed = jnp.einsum(
            "qjn,nd->qjd", weights.astype(jnp.bfloat16), values, preferred_element_type=jnp.float32
        ) + jnp.einsum(
            "qjs,qsd->qjd",
            tail_weights.astype(jnp.bfloat16),
            suffix[:, :, 1, g],
            preferred_element_type=jnp.float32,
        )
        answers.append((mixed / totals).astype(jnp.bfloat16))
    return jnp.stack(answers, axis=1).reshape(quest_count, -1)


def solution(mesh):
    placed = (
        P("seq", None),
        P(),
        P("seq", None, "head"),
        P("head", "seq"),
        P("seq", None),
        P(),
        P("seq", None, "head"),
        P("seq", "head"),
        P("seq", None, None, "head"),
        P("seq"),
        P(),
    )
    return jax.shard_map(
        on_device, mesh=mesh, in_specs=placed, out_specs=P("seq", "head"), check_vma=False
    )
```

```python
import functools

import jax
import jax.numpy as jnp
from jax import lax
from jax.experimental import pallas as pl
from jax.experimental.pallas import tpu as pltpu
from jax.sharding import PartitionSpec as P

VD = 1280
VH = 16
HD = 128
FPATCH = 256
WIN = 64

MESH = pl.DeviceIdType.MESH
VMEM = pl.BlockSpec(memory_space=pltpu.VMEM)


def rms_scale(values, gain):
    return values * lax.rsqrt(jnp.mean(values * values, axis=-1, keepdims=True) + 1e-06) * gain


def exchange_kernel(axis, count, gather, x_ref, out_ref, send_sem, recv_sem, own_sem):
    me = lax.axis_index(axis)
    barrier = pltpu.get_barrier_semaphore()
    for step in range(1, count):
        pl.semaphore_signal(
            barrier, inc=1, device_id={axis: lax.rem(me + step, count)}, device_id_type=MESH
        )
    pl.semaphore_wait(barrier, count - 1)
    copies = []
    for step in range(1, count):
        peer = lax.rem(me + step, count)
        copy = pltpu.make_async_remote_copy(
            src_ref=x_ref if gather else x_ref.at[peer],
            dst_ref=out_ref.at[me],
            send_sem=send_sem.at[step],
            recv_sem=recv_sem.at[step],
            device_id={axis: peer},
            device_id_type=MESH,
        )
        copy.start()
        copies.append(copy)
    own = pltpu.make_async_copy(x_ref if gather else x_ref.at[me], out_ref.at[me], own_sem)
    own.start()
    own.wait()
    for copy in copies:
        copy.wait()


def exchange(x, axis, gather, collective_id):
    count = lax.axis_size(axis)
    shape = ((count,) + x.shape) if gather else x.shape
    return pl.pallas_call(
        functools.partial(exchange_kernel, axis, count, gather),
        out_shape=jax.ShapeDtypeStruct(shape, x.dtype),
        in_specs=[VMEM],
        out_specs=VMEM,
        scratch_shapes=[
            pltpu.SemaphoreType.DMA((count,)),
            pltpu.SemaphoreType.DMA((count,)),
            pltpu.SemaphoreType.DMA,
        ],
        compiler_params=pltpu.CompilerParams(collective_id=collective_id, has_side_effects=True),
        name=f"exchange_{collective_id}",
    )(x)


def ring_kernel(count, sizes, *refs):
    arrays = len(sizes)
    ins, outs = refs[:arrays], refs[arrays : 2 * arrays]
    send_sem, recv_sem, own_sem = refs[2 * arrays :]
    places = [(a, i) for a, size in enumerate(sizes) for i in range(size)]
    me = lax.axis_index("seq")
    odd = lax.rem(me, 2)
    place = (1 - odd) * (me // 2) + odd * (count - 1 - me // 2)

    def index_of(position):
        position = lax.rem(position + count, count)
        late = position // (count // 2)
        return (1 - late) * 2 * position + late * (2 * (count - 1 - position) + 1)

    neighbours = (index_of(place + 1), index_of(place - 1))
    barrier = pltpu.get_barrier_semaphore()
    for neighbour in neighbours:
        pl.semaphore_signal(barrier, inc=1, device_id={"seq": neighbour}, device_id_type=MESH)
    pl.semaphore_wait(barrier, 2)
    far, near = count // 2, count - 1 - count // 2
    pieces = len(places)

    def slot(piece, source):
        a, i = places[piece]
        return outs[a].at[i, source]

    def own(piece):
        a, i = places[piece]
        return ins[a].at[i]

    copies = {}
    for step in range(far):
        for piece in range(pieces):
            for way in range(2):
                hops = far if (piece < 2) == (way == 0) else near
                if step >= hops:
                    continue
                source = index_of(place - step if way == 0 else place + step)
                if step > 0:
                    copies[step - 1, piece, way].wait_recv()
                copy = pltpu.make_async_remote_copy(
                    src_ref=own(piece) if step == 0 else slot(piece, source),
                    dst_ref=slot(piece, source),
                    send_sem=send_sem.at[step, piece, way],
                    recv_sem=recv_sem.at[step, piece, way],
                    device_id={"seq": neighbours[way]},
                    device_id_type=MESH,
                )
                copy.start()
                copies[step, piece, way] = copy
    kept = [pltpu.make_async_copy(own(p), slot(p, me), own_sem.at[p]) for p in range(pieces)]
    for copy in kept:
        copy.start()
    for copy in kept:
        copy.wait()
    for (step, piece, way), copy in copies.items():
        if (step + 1, piece, way) not in copies:
            copy.wait_recv()
    for copy in copies.values():
        copy.wait_send()


def ring_gather(arrays, collective_id):
    count = lax.axis_size("seq")
    far = count // 2
    sizes = tuple(x.shape[0] for x in arrays)
    pieces = sum(sizes)
    return pl.pallas_call(
        functools.partial(ring_kernel, count, sizes),
        out_shape=tuple(
            jax.ShapeDtypeStruct((x.shape[0], count) + x.shape[1:], x.dtype) for x in arrays
        ),
        in_specs=[VMEM] * len(arrays),
        out_specs=(VMEM,) * len(arrays),
        scratch_shapes=[
            pltpu.SemaphoreType.DMA((far, pieces, 2)),
            pltpu.SemaphoreType.DMA((far, pieces, 2)),
            pltpu.SemaphoreType.DMA((pieces,)),
        ],
        compiler_params=pltpu.CompilerParams(collective_id=collective_id, has_side_effects=True),
        name=f"ring_gather_{collective_id}",
    )(*arrays)


def frame_attention(query, key, value, unit_order, head_size):
    unit_count = unit_order.shape[0]
    patch_count = unit_count * 4
    ranks = jnp.sum(
        jnp.where(
            unit_order[None, :] == (jnp.arange(patch_count) // 4)[:, None],
            jnp.arange(unit_count)[None, :] // (WIN // 4),
            0,
        ),
        axis=1,
    )
    same = ranks[:, None] == ranks[None, :]
    scores = jnp.einsum(
        "qhd,khd->hqk", query, key, preferred_element_type=jnp.float32
    ) * head_size ** (-0.5)
    scores = jnp.where(same[None], scores, -jnp.inf)
    weights = jax.nn.softmax(scores, axis=-1).astype(jnp.bfloat16)
    return jnp.einsum(
        "hqk,khd->qhd", weights, value, preferred_element_type=jnp.float32
    ).astype(jnp.bfloat16)


def on_device(
    patches,
    norm_gain,
    w_qkv,
    w_out,
    window_order,
    merge_gain,
    w_kv,
    queries,
    suffix_kv,
    question_lengths,
    frame_range,
):
    head_count = lax.axis_size("head")
    seq_count = lax.axis_size("seq")
    row_count = patches.shape[0]
    frame_count = window_order.shape[0]
    columns = w_qkv.shape[2]
    head_size = VD // VH
    local_heads = columns // head_size
    source = patches.astype(jnp.float32)
    normed = rms_scale(source, norm_gain).astype(jnp.bfloat16)
    qkv_all, w_out_all = ring_gather((w_qkv.transpose(1, 0, 2), w_out.T[None]), 0)
    qkv_all = qkv_all.reshape(3, -1, columns)
    query, key, value = [
        jnp.dot(normed, qkv_all[part], preferred_element_type=jnp.float32)
        .astype(jnp.bfloat16)
        .reshape(frame_count, -1, local_heads, head_size)
        for part in range(3)
    ]
    attended = jax.vmap(
        lambda q, k, v, order: frame_attention(q, k, v, order, head_size)
    )(query, key, value, window_order).reshape(row_count, columns)
    w_full = w_out_all.reshape(VD, columns)
    share_rows = row_count // head_count
    partial = jnp.einsum(
        "rc,oc->ro", attended, w_full, preferred_element_type=jnp.float32
    ).astype(jnp.bfloat16)
    parts = exchange(partial.reshape(head_count, share_rows, VD), "head", False, 1)
    shared = jnp.sum(parts.astype(jnp.float32), axis=0)
    own_rows = lax.dynamic_slice_in_dim(source, lax.axis_index("head") * share_rows, share_rows, 0)
    merged = rms_scale(own_rows + shared, merge_gain).astype(jnp.bfloat16)
    share_tokens = share_rows // 4
    depth = w_kv.shape[0]
    merged = merged.reshape(share_tokens, seq_count, depth).transpose(1, 0, 2)
    merged = exchange(merged, "seq", False, 2)
    merged = exchange(merged, "head", True, 3)
    merged = merged.transpose(1, 0, 2, 3).reshape(-1, depth)
    kv_columns = w_kv.shape[2]
    partial = jnp.dot(
        merged, w_kv.reshape(depth, 2 * kv_columns), preferred_element_type=jnp.float32
    )
    parts = exchange(partial.reshape(seq_count, -1, 2 * kv_columns), "seq", False, 4)
    visual = jnp.sum(parts, axis=0).astype(jnp.bfloat16)
    pieces = 4
    (visual,) = ring_gather((visual.reshape(pieces, -1, 2 * kv_columns),), 5)
    visual = visual.reshape(-1, 2 * kv_columns)

    token_count = visual.shape[0]
    quest_count = queries.shape[0]
    span = suffix_kv.shape[1]
    kv_local = kv_columns // HD
    asking = queries.reshape(quest_count, kv_local, -1, HD)
    frame_tokens = FPATCH // 4
    seq_index = lax.axis_index("seq")
    bounds = lax.dynamic_slice_in_dim(frame_range, seq_index * quest_count, quest_count, 0)
    token_index = jnp.arange(token_count).reshape(seq_count, pieces, -1).transpose(1, 0, 2)
    frame_index = token_index.reshape(-1) // frame_tokens
    live = (frame_index[None, :] >= bounds[:, 0:1]) & (frame_index[None, :] < bounds[:, 1:2])
    suffix_live = jnp.arange(span)[None, :] < question_lengths[:, None]
    suffix = suffix_kv.reshape(quest_count, span, 2, kv_local, HD)
    answers = []
    for g in range(kv_local):
        ask = asking[:, g]
        keys = visual[:, g * HD : (g + 1) * HD]
        values = visual[:, kv_columns + g * HD : kv_columns + (g + 1) * HD]
        scores = jnp.einsum(
            "qjd,nd->qjn", ask, keys, preferred_element_type=jnp.float32
        ) * HD ** (-0.5)
        scores = jnp.where(live[:, None, :], scores, -jnp.inf)
        tail = jnp.einsum(
            "qjd,qsd->qjs", ask, suffix[:, :, 0, g], preferred_element_type=jnp.float32
        ) * HD ** (-0.5)
        tail = jnp.where(suffix_live[:, None, :], tail, -jnp.inf)
        highest = jnp.maximum(
            jnp.max(scores, axis=-1, keepdims=True), jnp.max(tail, axis=-1, keepdims=True)
        )
        weights = jnp.exp(scores - highest)
        tail_weights = jnp.exp(tail - highest)
        totals = jnp.sum(weights, axis=-1, keepdims=True) + jnp.sum(
            tail_weights, axis=-1, keepdims=True
        )
        mixed = jnp.einsum(
            "qjn,nd->qjd", weights.astype(jnp.bfloat16), values, preferred_element_type=jnp.float32
        ) + jnp.einsum(
            "qjs,qsd->qjd",
            tail_weights.astype(jnp.bfloat16),
            suffix[:, :, 1, g],
            preferred_element_type=jnp.float32,
        )
        answers.append((mixed / totals).astype(jnp.bfloat16))
    return jnp.stack(answers, axis=1).reshape(quest_count, -1)


def solution(mesh):
    placed = (
        P("seq", None),
        P(),
        P("seq", None, "head"),
        P("head", "seq"),
        P("seq", None),
        P(),
        P("seq", None, "head"),
        P("seq", "head"),
        P("seq", None, None, "head"),
        P("seq"),
        P(),
    )
    return jax.shard_map(
        on_device, mesh=mesh, in_specs=placed, out_specs=P("seq", "head"), check_vma=False
    )
```
